32 devices in a mesh: parts: 2 (over y), sub: 4 (over z), row: 2 (over x), col: 2 (over core).
Axes of the slice: x: 2, y: 2, z: 4, core: 2. Of those that a mesh axis runs over, the one named last changes fastest.
Arguments:
- loads: float32 [8, 32, 1024], P(('parts', 'sub'), 'col'), parts along dimension 0, may hold values from -6 to 6
- weights: float32 [8, 1024], P(('parts', 'sub')), parts along dimension 0, may hold values from 0.25 to 4
- dual_ops: bfloat16 [8, 2048, 2048], P(('parts', 'sub'), 'row'), parts along dimension 0, as said below
- corner_maps: bfloat16 [8, 24, 2048], P(('parts', 'sub'), None, 'row'), parts along dimension 0, may hold values from -0.25 to 0.25
- coarse_inverse: float32 [96, 48], P('parts'), parts along dimension 0, as said below
- corner_ids: int32 [8, 24], P('parts'), parts along dimension 0, may hold values from 0 to 47, as said below
- iface_sizes: int32 [8], P('parts'), parts along dimension 0, may hold values from 512 to 1024, as said below
- left_partner: int32 [8, 1024], P(('parts', 'sub')), parts along dimension 0, may hold values from 0 to 1023, as said below
- right_partner: int32 [8, 1024], P(('parts', 'sub')), parts along dimension 0, may hold values from 0 to 1023, as said below
Outputs:
- solution: float32 [8, 32, 1024], P(('parts', 'sub'), 'col'), parts along dimension 0
- residual: float32 [8, 32, 1024], P(('parts', 'sub'), 'col'), parts along dimension 0
The draws below stay inside these ranges and needn't reach their ends.
There are 2 independent parts, one for each index of `parts`. The reference program is written for one: setup_inputs(seed, part) draws one part's arguments, and reference() takes and returns one part's arrays. A program takes and returns all parts, laid end to end along the dimension named above; each array names one. Nothing has to cross between parts.
Inputs may be any that keep to these rules, and one draw needn't show every extreme that they name: Global indices 24/2 * s to 24/2 * s + 24/2 - 1 are the corners of the interface between s and s+1; the first half of subdomain s's corner_ids is a permutation of those of interface s-1, the second half a permutation of those of interface s. `left_partner`: each row s is a permutation that maps the slots below iface_sizes[s-1] onto slots below it. `right_partner`: each row s is a permutation that maps the slots below iface_sizes[s] onto slots below it, and is the inverse of left_partner[s+1]. `dual_ops`: symmetric positive definite. `coarse_inverse`: symmetric positive definite. For each s < 2, one of iface_sizes[s] and iface_sizes[s + 2] is 896 or more and the other 640 or less.
All inputs are finite; a program needn't handle non-finite values.
Results may differ from the reference program's by a relative error of at most 0.015.
Values may be sent and summed in bfloat16 or wider, within the bound.
A program may use at most 64 MiB of HBM per device.

```python
import math
import jax
import jax.numpy as jnp
from jax import lax

ORDER = 2048
COLS = 32
C_LOC = 24
ITERS = 2
S = 4
HALF = 1024
NC = 48


def draw_dual_ops(key, part):

    def one_matrix(sub_key):
        first, second = jax.random.split(sub_key)
        noise = jax.random.normal(first, (ORDER, ORDER), jnp.float32)
        spread = 0.35
        diagonal = jax.random.uniform(second, (ORDER,), jnp.float32, 1.0, 3.0)
        symmetric = (noise + noise.T) * (spread / (2.0 * ORDER) ** 0.5)
        return (symmetric + jnp.diag(diagonal)).astype(jnp.bfloat16)
    return lax.map(one_matrix, jax.random.split(key, S))


def draw_coarse_inverse(key, part):
    first, second = jax.random.split(jax.random.fold_in(key, 3))
    noise = jax.random.normal(first, (NC, NC), jnp.float32)
    spread = 0.5
    diagonal = jax.random.uniform(second, (NC,), jnp.float32, 1.5, 3.0)
    symmetric = (noise + noise.T) * (spread / (2.0 * NC) ** 0.5)
    return symmetric + jnp.diag(diagonal)


def draw_corner_ids(key, part):
    width = C_LOC // 2
    keys = jax.random.split(jax.random.fold_in(key, 5), 2 * S)
    orders = jax.vmap(lambda one_key: jax.random.permutation(one_key, width))(keys).astype(jnp.int32)
    subdomains = jnp.arange(S, dtype=jnp.int32)
    before = width * ((subdomains + S - 1) % S)[:, None] + orders[:S]
    after = width * subdomains[:, None] + orders[S:]
    return jnp.concatenate([before, after], axis=1).astype(jnp.int32)


def interface_sizes(key):
    first, second, third = jax.random.split(jax.random.fold_in(key, 11), 3)
    pairs = S // 2
    light = jax.random.randint(first, (pairs,), HALF // 2, 5 * HALF // 8 + 1, dtype=jnp.int32)
    heavy = jax.random.randint(second, (pairs,), 7 * HALF // 8, HALF + 1, dtype=jnp.int32)
    flip = jax.random.randint(third, (pairs,), 0, 2, dtype=jnp.int32)
    lower = jnp.where(flip == 1, heavy, light)
    upper = jnp.where(flip == 1, light, heavy)
    return jnp.concatenate([lower, upper]).astype(jnp.int32)


def draw_iface_sizes(key, part):
    return interface_sizes(key)


def interface_orders(key):
    sizes = interface_sizes(key)
    keys = jax.random.split(jax.random.fold_in(key, 7), S)
    slots = jnp.arange(HALF, dtype=jnp.int32)

    def one_order(one_key, count):
        ranks = jax.random.permutation(one_key, HALF).astype(jnp.int32)
        scores = ranks + HALF * (slots >= count).astype(jnp.int32)
        return jnp.argsort(scores, stable=True).astype(jnp.int32)
    return jax.vmap(one_order)(keys, sizes).astype(jnp.int32)


def draw_left_partner(key, part):
    return jnp.roll(interface_orders(key), 1, axis=0).astype(jnp.int32)


def draw_right_partner(key, part):
    return jnp.argsort(interface_orders(key), axis=1, stable=True).astype(jnp.int32)


def block_scale(key, extent, shards, least, largest):
    level, own = 1.0, jax.random.fold_in(key, 6)
    for dim, blocks in shards:
        steps = jnp.exp(jax.random.uniform(jax.random.fold_in(own, dim), (blocks,), jnp.float32, least / len(shards), largest / len(shards)))
        level = level * jnp.repeat(steps, extent[dim] // blocks).reshape([-1 if axis == dim else 1 for axis in range(len(extent))])
    return level


def centred(stream_key, dims, scale, reach, cuts=(), kind=jnp.bfloat16):
    level = block_scale(stream_key, dims, cuts, -0.22, 0.18) if cuts else 1.0
    entries = jax.random.normal(stream_key, dims, jnp.float32) * scale * level
    return jnp.minimum(jnp.maximum(entries, -reach), reach).astype(kind)


def setup_inputs(seed: int = 0, part: int = 0) -> dict:
    key_of = jax.random.split(jax.random.key(seed), 10)
    part_keys = jax.random.split(jax.random.fold_in(key_of[9], part), 10)
    return {
        "loads": centred(part_keys[0], (S, COLS, HALF), 1.0, 6.0, ((0, 4), (1, 2)), jnp.float32),
        "weights": jnp.clip(jnp.exp(math.log(4.0) - 2.7725887 * jax.random.uniform(part_keys[1], (S, HALF), jnp.float32) ** block_scale(part_keys[1], (S, HALF), ((0, 4),), -0.2, 0.2)), 0.25, 4.0),
        "dual_ops": draw_dual_ops(jax.random.fold_in(jax.random.fold_in(key_of[9], part), 71), part),
        "corner_maps": centred(part_keys[3], (S, C_LOC, ORDER), (ORDER // 4) ** -0.5, 0.25, ((0, 4), (2, 2))),
        "coarse_inverse": draw_coarse_inverse(jax.random.fold_in(jax.random.fold_in(key_of[9], part), 71), part),
        "corner_ids": draw_corner_ids(jax.random.fold_in(jax.random.fold_in(key_of[9], part), 71), part),
        "iface_sizes": draw_iface_sizes(jax.random.fold_in(jax.random.fold_in(key_of[9], part), 71), part),
        "left_partner": draw_left_partner(jax.random.fold_in(jax.random.fold_in(key_of[9], part), 71), part),
        "right_partner": draw_right_partner(jax.random.fold_in(jax.random.fold_in(key_of[9], part), 71), part),
    }


def apply_operator(vec, dual_ops, corner_maps, coarse_inverse, corner_ids, left_partner, right_partner, live):
    ahead = jnp.roll(vec, -1, axis=0)
    right_index = jnp.broadcast_to(right_partner[:, None, :], vec.shape)
    right_side = jnp.take_along_axis(ahead, right_index, axis=2)
    full = jnp.concatenate([vec, right_side], axis=2).astype(jnp.bfloat16)

    def one_local(items):
        piece, matrix, coupling = items
        local = jnp.dot(piece, matrix, preferred_element_type=jnp.float32)
        corner = jnp.dot(piece, coupling.T, preferred_element_type=jnp.float32)
        return local, corner

    local, corner = lax.map(one_local, (full, dual_ops, corner_maps))
    columns = jnp.arange(NC, dtype=jnp.int32)
    onehot = (corner_ids[:, :, None] == columns[None, None, :]).astype(jnp.float32)
    coarse = jnp.einsum("scj,sjn->cn", corner, onehot, precision=lax.Precision.HIGHEST)
    solved = jnp.dot(coarse, coarse_inverse, precision=lax.Precision.HIGHEST)
    back = jnp.einsum("cn,sjn->scj", solved, onehot, precision=lax.Precision.HIGHEST).astype(jnp.bfloat16)

    def one_back(items):
        piece, coupling = items
        return jnp.dot(piece, coupling, preferred_element_type=jnp.float32)

    united = local + lax.map(one_back, (back, corner_maps))
    upper = jnp.roll(united[:, :, HALF:], 1, axis=0)
    left_index = jnp.broadcast_to(left_partner[:, None, :], vec.shape)
    return (united[:, :, :HALF] + jnp.take_along_axis(upper, left_index, axis=2)) * live[:, None, :]


def reference(loads, weights, dual_ops, corner_maps, coarse_inverse, corner_ids, iface_sizes, left_partner, right_partner):
    slots = jnp.arange(HALF, dtype=jnp.int32)
    live = (slots[None, :] < jnp.roll(iface_sizes, 1)[:, None]).astype(jnp.float32)
    scaling = weights[:, None, :]
    residual = loads * live[:, None, :]
    solution = jnp.zeros_like(residual)
    precond = scaling * residual
    direction = precond
    rz_value = jnp.sum(residual * precond, axis=(0, 2))
    for step in range(ITERS):
        image = apply_operator(direction, dual_ops, corner_maps, coarse_inverse, corner_ids, left_partner, right_partner, live)
        alpha = rz_value / jnp.sum(direction * image, axis=(0, 2))
        solution = solution + alpha[None, :, None] * direction
        residual = residual - alpha[None, :, None] * image
        precond = scaling * residual
        new_value = jnp.sum(residual * precond, axis=(0, 2))
        direction = precond + (new_value / rz_value)[None, :, None] * direction
        rz_value = new_value
    return solution, residual
```

```python
import functools

import jax
import jax.numpy as jnp
from jax import lax
from jax.experimental import pallas as pl
from jax.experimental.pallas import tpu as pltpu
from jax.sharding import PartitionSpec as P

MESH = pl.DeviceIdType.MESH
CHUNK = 256
BF = jnp.bfloat16
F32 = jnp.float32


def each(count, body):
    if count <= 8:
        for at in range(count):
            body(at)
    else:
        lax.fori_loop(0, count, lambda at, _: (body(at), 0)[1], 0)


def dot_nt(a, b):
    return lax.dot_general(a, b, (((1,), (1,)), ((), ())), preferred_element_type=F32)


def dot_nn(a, b):
    return lax.dot_general(a, b, (((1,), (0,)), ((), ())), preferred_element_type=F32)


def kernel(
    S, R, loads, weights, op, cm, cinv, ids, sizes, lmap, rmap, sol, res,
    loads_v, w_v, op_v, cv, cinv_p, ids_v, lmap_v, rmap_v,
    zsend, zrecv, wrecv, cmo, cmn, mo, mn, pl_m, pr_m, zs,
    own, nbr, pk,
    in_sem, op_sem, z_sem, cmo_ssem, cmo_rsem, cmn_ssem, cmn_rsem,
    own_ssem, own_rsem, nbr_ssem, nbr_rsem, pk_ssem, pk_rsem,
):
    s = lax.axis_index("sub")
    r = lax.axis_index("row")
    G = S * R
    me = s * R + r
    C, H = loads_v.shape
    B = op_v.shape[0]
    NC = cv.shape[0]
    W = cinv_p.shape[0]
    half_r = R // 2
    nxt = lax.rem(s + 1, S)
    prv = lax.rem(s + S - 1, S)
    side = r // half_r
    toward = lax.rem(s + S - 1 + 2 * side, S)

    ins = [
        pltpu.make_async_copy(src, dst, in_sem.at[i])
        for i, (src, dst) in enumerate([
            (loads.at[0], loads_v), (weights, w_v), (rmap, rmap_v), (lmap, lmap_v),
            (ids, ids_v), (cinv, cv), (cm.at[0], cmo.at[r]),
        ])
    ]
    for copy in ins:
        copy.start()
    chunk = min(CHUNK, B)
    ops = [
        pltpu.make_async_copy(
            op.at[0, pl.ds(c * chunk, chunk), :], op_v.at[pl.ds(c * chunk, chunk), :], op_sem.at[c]
        )
        for c in range(B // chunk)
    ]
    for copy in ops:
        copy.start()

    barrier = pltpu.get_barrier_semaphore()

    def peer(k):
        g = lax.rem(me + k + 1, G)
        return g, {"sub": g // R, "row": lax.rem(g, R)}

    def greet(k):
        _, who = peer(k)
        pl.semaphore_signal(barrier, inc=1, device_id=who, device_id_type=MESH)

    each(G - 1, greet)

    size_before = sizes[prv]
    size_after = sizes[s]
    lanes = lax.broadcasted_iota(jnp.int32, (1, H), 1)
    live_l = (lanes < size_before).astype(F32)
    ins[0].wait()
    ins[1].wait()
    w_l = w_v[...]
    r0 = loads_v[...] * live_l
    z0 = w_l * r0
    zsend[...] = z0.astype(BF)

    pl.semaphore_wait(barrier, G - 1)

    def remote(src, dst, ssem, rsem, who):
        return pltpu.make_async_remote_copy(
            src_ref=src, dst_ref=dst, send_sem=ssem, recv_sem=rsem, device_id=who, device_id_type=MESH
        )

    z_copy = remote(zsend, zrecv, z_sem.at[0], z_sem.at[1], {"sub": prv})
    w_copy = remote(weights, wrecv, z_sem.at[2], z_sem.at[3], {"sub": prv})
    z_copy.start()
    w_copy.start()

    def to_row(src, dst, ssem, rsem, k):
        q = lax.rem(r + k, R)
        return remote(src, dst.at[r], ssem.at[k], rsem.at[r], {"row": q})

    def to_side(src, dst, ssem, rsem, k):
        q = lax.rem(r + k, R)
        return remote(src, dst.at[r], ssem.at[k], rsem.at[r], {"sub": toward, "row": q})

    def wait_slot(dst, ssem, rsem, q):
        remote(dst.at[q], dst.at[q], ssem.at[0], rsem.at[q], {"sub": nxt}).wait_recv()

    cm_sends = [to_row(cm.at[0], cmo, cmo_ssem, cmo_rsem, k) for k in range(1, R)]
    cm_sends += [to_side(cm.at[0], cmn, cmn_ssem, cmn_rsem, k) for k in range(R)]
    for copy in cm_sends:
        copy.start()

    ins[2].wait()
    ins[3].wait()
    right_map = rmap_v[...]
    left_map = lmap_v[...]
    live_r = (right_map < size_after).astype(F32)

    def hot(target, the_map):
        step = 128
        for c in range(H // step):
            rows = lax.broadcasted_iota(jnp.int32, (step, H), 0) + c * step
            target[pl.ds(c * step, step), :] = (rows == the_map).astype(F32).astype(BF)

    hot(pr_m, right_map)
    hot(pl_m, left_map)
    ins[4].wait()
    ins[5].wait()
    cinv_p[...] = jnp.zeros_like(cinv_p)
    cinv_p[0:NC, 0:NC] = cv[...]

    def hot_ids(t):
        row = ids_v[pl.ds(t, 1), :]
        rows = lax.broadcasted_iota(jnp.int32, (W, row.shape[1]), 0)
        return (rows == row).astype(F32).astype(BF)

    hot_own = hot_ids(s)
    ins[6].wait()
    mo[r] = dot_nn(hot_own, cmo[r]).astype(BF)

    z_copy.wait_recv()
    w_copy.wait_recv()
    w_in = wrecv[...]
    w_hi = w_in.astype(BF)
    w_lo = (w_in - w_hi.astype(F32)).astype(BF)
    pad = lax.broadcasted_iota(jnp.int32, (16, H), 0)
    w_rows = jnp.where(pad == 0, w_hi.astype(F32), jnp.where(pad == 1, w_lo.astype(F32), 0.0))
    gathered = dot_nn(jnp.concatenate([zrecv[...], w_rows.astype(BF)], axis=0), pr_m[...])
    z0_r = gathered[:C]
    w_r = gathered[C : C + 1] + gathered[C + 1 : C + 2]

    col = lax.broadcasted_iota(jnp.int32, (C, W), 1)

    def pick(value, lane):
        return jnp.sum(jnp.where(col == lane, value, 0.0), axis=1, keepdims=True)

    def product(step, z_left, z_right, r_left):
        full = jnp.concatenate([z_left.astype(BF), z_right.astype(BF)], axis=1)
        for q in range(R):
            half = z_left if q < half_r else z_right
            at = (q % half_r) * B
            zs[q] = half[:, at : at + B]
        parts = []
        for c in range(B // chunk):
            if step == 0:
                ops[c].wait()
            parts.append(dot_nt(full, op_v[c * chunk : (c + 1) * chunk, :]))
        local = jnp.concatenate(parts, axis=1)
        own[step, r] = local.astype(BF)
        mine = own.at[step, r]
        sends = [
            to_side(mine, nbr.at[step], nbr_ssem.at[step], nbr_rsem.at[step], k) for k in range(R)
        ]
        sends += [
            to_row(mine, own.at[step], own_ssem.at[step], own_rsem.at[step], k) for k in range(1, R)
        ]
        for copy in sends:
            copy.start()
        block = zs[r]
        delta = jnp.sum(block * local, axis=1, keepdims=True)
        gamma = jnp.sum(r_left * z_left, axis=1, keepdims=True)
        gamma = jnp.where(r == 0, gamma, 0.0)
        corner = dot_nt(block.astype(BF), mo[r])
        packet = corner + jnp.where(col == NC, gamma, 0.0) + jnp.where(col == NC + 1, delta, 0.0)
        pk[step, me] = packet

        def spread(k):
            _, who = peer(k)
            remote(
                pk.at[step, me], pk.at[step, me], pk_ssem.at[step, k], pk_rsem.at[step, me], who
            ).start()

        each(G - 1, spread)
        return sends

    def collect(step, need_right):
        def arrive(k):
            g, who = peer(k)
            remote(
                pk.at[step, g], pk.at[step, g], pk_ssem.at[step, 0], pk_rsem.at[step, g], who
            ).wait_recv()

        each(G - 1, arrive)
        if G <= 8:
            total = pk[step, 0]
            for g in range(1, G):
                total = total + pk[step, g]
        else:
            total = lax.fori_loop(
                0, G, lambda g, acc: acc + pk[step, g], jnp.zeros((C, W), F32)
            )
        solved = lax.dot_general(
            total, cinv_p[...], (((1,), (0,)), ((), ())),
            precision=lax.Precision.HIGHEST, preferred_element_type=F32,
        )
        back = solved.astype(BF)
        gamma = pick(total, NC)
        delta = pick(total, NC + 1) + jnp.sum(total * back.astype(F32), axis=1, keepdims=True)
        for k in range(1, R):
            wait_slot(own.at[step], own_ssem.at[step], own_rsem.at[step], lax.rem(r + k, R))
        for q in range(R):
            wait_slot(nbr.at[step], nbr_ssem.at[step], nbr_rsem.at[step], q)

        def joined(store, maps, first, last):
            return jnp.concatenate(
                [store[step, q].astype(F32) + dot_nn(back, maps[q]) for q in range(first, last)], axis=1
            )

        from_prev = joined(nbr, mn, half_r, R).astype(BF)
        w_left = (joined(own, mo, 0, half_r) + dot_nn(from_prev, pl_m[...])) * live_l
        w_right = None
        if need_right:
            from_next = joined(nbr, mn, 0, half_r).astype(BF)
            w_right = (joined(own, mo, half_r, R) + dot_nn(from_next, pr_m[...])) * live_r
        return gamma, delta, w_left, w_right

    sends0 = product(0, z0, z0_r, r0)

    for k in range(1, R):
        q = lax.rem(r + k, R)
        wait_slot(cmo, cmo_ssem, cmo_rsem, q)
        mo[q] = dot_nn(hot_own, cmo[q]).astype(BF)
    hot_next = hot_ids(nxt)
    hot_prev = hot_ids(prv)
    for q in range(R):
        wait_slot(cmn, cmn_ssem, cmn_rsem, q)
        mn[q] = dot_nn(hot_next if q < half_r else hot_prev, cmn[q]).astype(BF)

    gamma0, delta0, wl0, wr0 = collect(0, True)
    alpha0 = gamma0 / delta0
    r1 = r0 - alpha0 * wl0
    z1 = w_l * r1
    z1_r = z0_r - alpha0 * (w_r * wr0)
    sends1 = product(1, z1, z1_r, r1)
    gamma1, delta1, wl1, _ = collect(1, False)
    beta = gamma1 / gamma0
    alpha1 = gamma1 / (delta1 - beta * gamma1 / alpha0)
    sol[...] = alpha0 * z0 + alpha1 * (z1 + beta * z0)
    res[...] = r1 - alpha1 * (wl1 + beta * wl0)

    z_copy.wait_send()
    w_copy.wait_send()
    for copy in cm_sends + sends0 + sends1:
        copy.wait_send()
    for step in range(2):

        def drain(k):
            _, who = peer(k)
            remote(
                pk.at[step, me], pk.at[step, me], pk_ssem.at[step, k], pk_rsem.at[step, me], who
            ).wait_send()

        each(G - 1, drain)


def per_device(S, R, loads, weights, dual_ops, corner_maps, coarse_inverse, corner_ids,
               iface_sizes, left_partner, right_partner):
    _, C, H = loads.shape
    _, B, full = dual_ops.shape
    J = corner_maps.shape[1]
    NC = coarse_inverse.shape[0]
    W = (NC + 2 + 127) // 128 * 128
    G = S * R
    DMA = pltpu.SemaphoreType.DMA
    anywhere = pl.BlockSpec(memory_space=pl.ANY)
    vmem = pl.BlockSpec(memory_space=pltpu.VMEM)
    out = jax.ShapeDtypeStruct((C, H), F32)
    sol, res = pl.pallas_call(
        functools.partial(kernel, S, R),
        out_shape=(out, out),
        in_specs=[anywhere] * 6 + [pl.BlockSpec(memory_space=pltpu.SMEM)] + [anywhere] * 2,
        out_specs=(vmem, vmem),
        scratch_shapes=[
            pltpu.VMEM((C, H), F32), pltpu.VMEM((1, H), F32), pltpu.VMEM((B, full), BF),
            pltpu.VMEM((NC, NC), F32), pltpu.VMEM((W, W), F32), pltpu.VMEM(corner_ids.shape, jnp.int32),
            pltpu.VMEM((1, H), jnp.int32), pltpu.VMEM((1, H), jnp.int32),
            pltpu.VMEM((C, H), BF), pltpu.VMEM((C, H), BF), pltpu.VMEM((1, H), F32),
            pltpu.VMEM((R, J, B), BF), pltpu.VMEM((R, J, B), BF),
            pltpu.VMEM((R, W, B), BF), pltpu.VMEM((R, W, B), BF),
            pltpu.VMEM((H, H), BF), pltpu.VMEM((H, H), BF), pltpu.VMEM((R, C, B), F32),
            pltpu.VMEM((2, R, C, B), BF), pltpu.VMEM((2, R, C, B), BF), pltpu.VMEM((2, G, C, W), F32),
            DMA((7,)), DMA((B // min(CHUNK, B),)), DMA((4,)), DMA((R,)), DMA((R,)), DMA((R,)), DMA((R,)),
            DMA((2, R)), DMA((2, R)), DMA((2, R)), DMA((2, R)), DMA((2, G)), DMA((2, G)),
        ],
        compiler_params=pltpu.CompilerParams(
            collective_id=0, has_side_effects=True, vmem_limit_bytes=48 * 1024 * 1024
        ),
    )(loads, weights, dual_ops, corner_maps, coarse_inverse, corner_ids, iface_sizes,
      left_partner, right_partner)
    return sol[None], res[None]


def solution(mesh):
    placed = (
        P(("parts", "sub"), "col", None),
        P(("parts", "sub"), None),
        P(("parts", "sub"), "row", None),
        P(("parts", "sub"), None, "row"),
        P("parts", None),
        P("parts", None),
        P("parts"),
        P(("parts", "sub"), None),
        P(("parts", "sub"), None),
    )
    return jax.shard_map(
        functools.partial(per_device, mesh.shape["sub"], mesh.shape["row"]),
        mesh=mesh,
        in_specs=placed,
        out_specs=(P(("parts", "sub"), "col", None), P(("parts", "sub"), "col", None)),
        check_vma=False,
    )
```

```python
import functools

import jax
import jax.numpy as jnp
from jax import lax
from jax.experimental import pallas as pl
from jax.experimental.pallas import tpu as pltpu
from jax.sharding import PartitionSpec as P

MESH = pl.DeviceIdType.MESH
CHUNK = 256
BF = jnp.bfloat16
F32 = jnp.float32


def each(count, body):
    if count <= 8:
        for at in range(count):
            body(at)
    else:
        lax.fori_loop(0, count, lambda at, _: (body(at), 0)[1], 0)


def dot_nt(a, b):
    return lax.dot_general(a, b, (((1,), (1,)), ((), ())), preferred_element_type=F32)


def dot_nn(a, b):
    return lax.dot_general(a, b, (((1,), (0,)), ((), ())), preferred_element_type=F32)


def kernel(
    S, R, loads, weights, op, cm, cinv, ids, sizes, lmap, rmap, sol, res,
    loads_v, w_v, op_v, cv, cinv_p, ids_v, lmap_v, rmap_v,
    zsend, zrecv, wrecv, cmo, cmn, mo, mn, pl_m, pr_m, zs,
    own, nbr, pk,
    in_sem, op_sem, z_sem, cmo_ssem, cmo_rsem, cmn_ssem, cmn_rsem,
    own_ssem, own_rsem, nbr_ssem, nbr_rsem, pk_ssem, pk_rsem,
):
    s = lax.axis_index("sub")
    r = lax.axis_index("row")
    G = S * R
    me = s * R + r
    C, H = loads_v.shape
    B = op_v.shape[0]
    NC = cv.shape[0]
    W = cinv_p.shape[0]
    half_r = R // 2
    nxt = lax.rem(s + 1, S)
    prv = lax.rem(s + S - 1, S)
    side = r // half_r
    toward = lax.rem(s + S - 1 + 2 * side, S)

    ins = [
        pltpu.make_async_copy(src, dst, in_sem.at[i])
        for i, (src, dst) in enumerate([
            (loads.at[0], loads_v), (weights, w_v), (rmap, rmap_v), (lmap, lmap_v),
            (ids, ids_v), (cinv, cv), (cm.at[0], cmo.at[r]),
        ])
    ]
    for copy in ins:
        copy.start()
    chunk = min(CHUNK, B)
    ops = [
        pltpu.make_async_copy(
            op.at[0, pl.ds(c * chunk, chunk), :], op_v.at[pl.ds(c * chunk, chunk), :], op_sem.at[c]
        )
        for c in range(B // chunk)
    ]
    for copy in ops:
        copy.start()

    barrier = pltpu.get_barrier_semaphore()

    def peer(k):
        g = lax.rem(me + k + 1, G)
        return g, {"sub": g // R, "row": lax.rem(g, R)}

    def greet(k):
        _, who = peer(k)
        pl.semaphore_signal(barrier, inc=1, device_id=who, device_id_type=MESH)

    each(G - 1, greet)

    size_before = sizes[prv]
    size_after = sizes[s]
    lanes = lax.broadcasted_iota(jnp.int32, (1, H), 1)
    live_l = (lanes < size_before).astype(F32)
    ins[0].wait()
    ins[1].wait()
    w_l = w_v[...]
    r0 = loads_v[...] * live_l
    z0 = w_l * r0
    zsend[...] = z0.astype(BF)

    pl.semaphore_wait(barrier, G - 1)

    def remote(src, dst, ssem, rsem, who):
        return pltpu.make_async_remote_copy(
            src_ref=src, dst_ref=dst, send_sem=ssem, recv_sem=rsem, device_id=who, device_id_type=MESH
        )

    z_copy = remote(zsend, zrecv, z_sem.at[0], z_sem.at[1], {"sub": prv})
    w_copy = remote(weights, wrecv, z_sem.at[2], z_sem.at[3], {"sub": prv})
    z_copy.start()
    w_copy.start()

    def to_row(src, dst, ssem, rsem, k):
        q = lax.rem(r + k, R)
        return remote(src, dst.at[r], ssem.at[k], rsem.at[r], {"row": q})

    def to_side(src, dst, ssem, rsem, k):
        q = lax.rem(r + k, R)
        return remote(src, dst.at[r], ssem.at[k], rsem.at[r], {"sub": toward, "row": q})

    def wait_slot(dst, ssem, rsem, q):
        remote(dst.at[q], dst.at[q], ssem.at[0], rsem.at[q], {"sub": nxt}).wait_recv()

    cm_sends = [to_row(cm.at[0], cmo, cmo_ssem, cmo_rsem, k) for k in range(1, R)]
    cm_sends += [to_side(cm.at[0], cmn, cmn_ssem, cmn_rsem, k) for k in range(R)]
    for copy in cm_sends:
        copy.start()

    ins[2].wait()
    ins[3].wait()
    right_map = rmap_v[...]
    left_map = lmap_v[...]
    live_r = (right_map < size_after).astype(F32)

    def hot(target, the_map):
        step = 128
        for c in range(H // step):
            rows = lax.broadcasted_iota(jnp.int32, (step, H), 0) + c * step
            target[pl.ds(c * step, step), :] = (rows == the_map).astype(F32).astype(BF)

    hot(pr_m, right_map)
    hot(pl_m, left_map)
    ins[4].wait()
    ins[5].wait()
    cinv_p[...] = jnp.zeros_like(cinv_p)
    cinv_p[0:NC, 0:NC] = cv[...]

    def hot_ids(t):
        row = ids_v[pl.ds(t, 1), :]
        rows = lax.broadcasted_iota(jnp.int32, (W, row.shape[1]), 0)
        return (rows == row).astype(F32).astype(BF)

    hot_own = hot_ids(s)
    ins[6].wait()
    mo[r] = dot_nn(hot_own, cmo[r]).astype(BF)

    z_copy.wait_recv()
    w_copy.wait_recv()
    w_in = wrecv[...]
    w_hi = w_in.astype(BF)
    w_lo = (w_in - w_hi.astype(F32)).astype(BF)
    pad = lax.broadcasted_iota(jnp.int32, (16, H), 0)
    w_rows = jnp.where(pad == 0, w_hi.astype(F32), jnp.where(pad == 1, w_lo.astype(F32), 0.0))
    gathered = dot_nn(jnp.concatenate([zrecv[...], w_rows.astype(BF)], axis=0), pr_m[...])
    z0_r = gathered[:C]
    w_r = gathered[C : C + 1] + gathered[C + 1 : C + 2]

    col = lax.broadcasted_iota(jnp.int32, (C, W), 1)

    def pick(value, lane):
        return jnp.sum(jnp.where(col == lane, value, 0.0), axis=1, keepdims=True)

    def product(step, z_left, z_right, r_left):
        full = jnp.concatenate([z_left.astype(BF), z_right.astype(BF)], axis=1)
        for q in range(R):
            half = z_left if q < half_r else z_right
            at = (q % half_r) * B
            zs[q] = half[:, at : at + B]
        parts = []
        for c in range(B // chunk):
            if step == 0:
                ops[c].wait()
            parts.append(dot_nt(full, op_v[c * chunk : (c + 1) * chunk, :]))
        local = jnp.concatenate(parts, axis=1)
        own[step, r] = local.astype(BF)
        mine = own.at[step, r]
        sends = [
            to_side(mine, nbr.at[step], nbr_ssem.at[step], nbr_rsem.at[step], k) for k in range(R)
        ]
        sends += [
            to_row(mine, own.at[step], own_ssem.at[step], own_rsem.at[step], k) for k in range(1, R)
        ]
        for copy in sends:
            copy.start()
        block = zs[r]
        delta = jnp.sum(block * local, axis=1, keepdims=True)
        gamma = jnp.sum(r_left * z_left, axis=1, keepdims=True)
        gamma = jnp.where(r == 0, gamma, 0.0)
        corner = dot_nt(block.astype(BF), mo[r])
        packet = corner + jnp.where(col == NC, gamma, 0.0) + jnp.where(col == NC + 1, delta, 0.0)
        pk[step, me] = packet

        def spread(k):
            _, who = peer(k)
            remote(
                pk.at[step, me], pk.at[step, me], pk_ssem.at[step, k], pk_rsem.at[step, me], who
            ).start()

        each(G - 1, spread)
        return sends

    def collect(step, need_right):
        def arrive(k):
            g, who = peer(k)
            remote(
                pk.at[step, g], pk.at[step, g], pk_ssem.at[step, 0], pk_rsem.at[step, g], who
            ).wait_recv()

        each(G - 1, arrive)
        if G <= 8:
            total = pk[step, 0]
            for g in range(1, G):
                total = total + pk[step, g]
        else:
            total = lax.fori_loop(
                0, G, lambda g, acc: acc + pk[step, g], jnp.zeros((C, W), F32)
            )
        solved = lax.dot_general(
            total, cinv_p[...], (((1,), (0,)), ((), ())),
            precision=lax.Precision.HIGHEST, preferred_element_type=F32,
        )
        back = solved.astype(BF)
        gamma = pick(total, NC)
        delta = pick(total, NC + 1) + jnp.sum(total * back.astype(F32), axis=1, keepdims=True)
        for k in range(1, R):
            wait_slot(own.at[step], own_ssem.at[step], own_rsem.at[step], lax.rem(r + k, R))
        for q in range(R):
            wait_slot(nbr.at[step], nbr_ssem.at[step], nbr_rsem.at[step], q)

        def joined(store, maps, first, last):
            return jnp.concatenate(
                [store[step, q].astype(F32) + dot_nn(back, maps[q]) for q in range(first, last)], axis=1
            )

        from_prev = joined(nbr, mn, half_r, R).astype(BF)
        w_left = (joined(own, mo, 0, half_r) + dot_nn(from_prev, pl_m[...])) * live_l
        w_right = None
        if need_right:
            from_next = joined(nbr, mn, 0, half_r).astype(BF)
            w_right = (joined(own, mo, half_r, R) + dot_nn(from_next, pr_m[...])) * live_r
        return gamma, delta, w_left, w_right

    sends0 = product(0, z0, z0_r, r0)

    for k in range(1, R):
        q = lax.rem(r + k, R)
        wait_slot(cmo, cmo_ssem, cmo_rsem, q)
        mo[q] = dot_nn(hot_own, cmo[q]).astype(BF)
    hot_next = hot_ids(nxt)
    hot_prev = hot_ids(prv)
    for q in range(R):
        wait_slot(cmn, cmn_ssem, cmn_rsem, q)
        mn[q] = dot_nn(hot_next if q < half_r else hot_prev, cmn[q]).astype(BF)

    gamma0, delta0, wl0, wr0 = collect(0, True)
    alpha0 = gamma0 / delta0
    r1 = r0 - alpha0 * wl0
    z1 = w_l * r1
    z1_r = z0_r - alpha0 * (w_r * wr0)
    sends1 = product(1, z1, z1_r, r1)
    gamma1, delta1, wl1, _ = collect(1, False)
    beta = gamma1 / gamma0
    alpha1 = gamma1 / (delta1 - beta * gamma1 / alpha0)
    sol[...] = alpha0 * z0 + alpha1 * (z1 + beta * z0)
    res[...] = r1 - alpha1 * (wl1 + beta * wl0)

    z_copy.wait_send()
    w_copy.wait_send()
    for copy in cm_sends + sends0 + sends1:
        copy.wait_send()
    for step in range(2):

        def drain(k):
            _, who = peer(k)
            remote(
                pk.at[step, me], pk.at[step, me], pk_ssem.at[step, k], pk_rsem.at[step, me], who
            ).wait_send()

        each(G - 1, drain)


def per_device(S, R, loads, weights, dual_ops, corner_maps, coarse_inverse, corner_ids,
               iface_sizes, left_partner, right_partner):
    _, C, H = loads.shape
    _, B, full = dual_ops.shape
    J = corner_maps.shape[1]
    NC = coarse_inverse.shape[0]
    W = (NC + 2 + 127) // 128 * 128
    G = S * R
    DMA = pltpu.SemaphoreType.DMA
    anywhere = pl.BlockSpec(memory_space=pltpu.HBM)
    vmem = pl.BlockSpec(memory_space=pltpu.VMEM)
    out = jax.ShapeDtypeStruct((C, H), F32)
    sol, res = pl.pallas_call(
        functools.partial(kernel, S, R),
        out_shape=(out, out),
        in_specs=[anywhere] * 6 + [pl.BlockSpec(memory_space=pltpu.SMEM)] + [anywhere] * 2,
        out_specs=(vmem, vmem),
        scratch_shapes=[
            pltpu.VMEM((C, H), F32), pltpu.VMEM((1, H), F32), pltpu.VMEM((B, full), BF),
            pltpu.VMEM((NC, NC), F32), pltpu.VMEM((W, W), F32), pltpu.VMEM(corner_ids.shape, jnp.int32),
            pltpu.VMEM((1, H), jnp.int32), pltpu.VMEM((1, H), jnp.int32),
            pltpu.VMEM((C, H), BF), pltpu.VMEM((C, H), BF), pltpu.VMEM((1, H), F32),
            pltpu.VMEM((R, J, B), BF), pltpu.VMEM((R, J, B), BF),
            pltpu.VMEM((R, W, B), BF), pltpu.VMEM((R, W, B), BF),
            pltpu.VMEM((H, H), BF), pltpu.VMEM((H, H), BF), pltpu.VMEM((R, C, B), F32),
            pltpu.VMEM((2, R, C, B), BF), pltpu.VMEM((2, R, C, B), BF), pltpu.VMEM((2, G, C, W), F32),
            DMA((7,)), DMA((B // min(CHUNK, B),)), DMA((4,)), DMA((R,)), DMA((R,)), DMA((R,)), DMA((R,)),
            DMA((2, R)), DMA((2, R)), DMA((2, R)), DMA((2, R)), DMA((2, G)), DMA((2, G)),
        ],
        compiler_params=pltpu.CompilerParams(
            collective_id=0, has_side_effects=True, vmem_limit_bytes=67_043_328
        ),
    )(loads, weights, dual_ops, corner_maps, coarse_inverse, corner_ids, iface_sizes,
      left_partner, right_partner)
    return sol[None], res[None]


def solution(mesh):
    placed = (
        P(("parts", "sub"), "col", None),
        P(("parts", "sub"), None),
        P(("parts", "sub"), "row", None),
        P(("parts", "sub"), None, "row"),
        P("parts", None),
        P("parts", None),
        P("parts"),
        P(("parts", "sub"), None),
        P(("parts", "sub"), None),
    )
    return jax.shard_map(
        functools.partial(per_device, mesh.shape["sub"], mesh.shape["row"]),
        mesh=mesh,
        in_specs=placed,
        out_specs=(P(("parts", "sub"), "col", None), P(("parts", "sub"), "col", None)),
        check_vma=False,
    )
```
